8 devices in a mesh: dp: 1 (over z), tp: 8 (over x, y, core).
Axes of the slice: x: 2, y: 2, z: 1, core: 2. Of those that a mesh axis runs over, the one named last changes fastest.
Arguments:
- x: bfloat16 [1024, 12288], P(('dp', 'tp'))
- gain_a: bfloat16 [12288], replicated
- wq: bfloat16 [12288, 12288], P(None, 'tp')
- wk: bfloat16 [12288, 1024], P(None, 'tp')
- wv: bfloat16 [12288, 1024], P(None, 'tp')
- wo: bfloat16 [12288, 12288], P('tp')
- gain_m: bfloat16 [12288], replicated
- w_gate: bfloat16 [12288, 28672], P(None, 'tp')
- w_up: bfloat16 [12288, 28672], P(None, 'tp')
- w_down: bfloat16 [28672, 12288], P('tp')
Outputs:
- output: bfloat16 [1024, 12288], P(('dp', 'tp'))
All inputs are finite; a program needn't handle non-finite values.
Results may differ from the reference program's by a relative error of at most 0.017.
Values are sent between devices in bfloat16 or wider.
A program may use at most 2 GiB of HBM per device.

```python
import jax
import jax.numpy as jnp
from jax import lax

ROWS = 1024
D = 12288
HEADS = 96
KV_HEADS = 8
HEAD = 128
FF = 28672
THETA = 10000


def setup_inputs(seed: int = 0, part: int = 0) -> dict:
    kx, kn, kq, kk, kv, ko, km, kg, ku, kd = jax.random.split(jax.random.key(seed), 10)

    def weights(key, rows, columns):
        return jax.random.normal(key, (rows, columns), jnp.float32) * rows**-0.5

    drawn = {
        "x": jax.random.normal(jax.random.fold_in(kx, part), (ROWS, D), jnp.float32),
        "gain_a": 1 + 0.1 * jax.random.normal(kn, (D,), jnp.float32),
        "wq": 2 * weights(kq, D, HEADS * HEAD),
        "wk": 2 * weights(kk, D, KV_HEADS * HEAD),
        "wv": 4 * weights(kv, D, KV_HEADS * HEAD),
        "wo": weights(ko, HEADS * HEAD, D),
        "gain_m": 1 + 0.1 * jax.random.normal(km, (D,), jnp.float32),
        "w_gate": weights(kg, D, FF),
        "w_up": weights(ku, D, FF),
        "w_down": 2 * weights(kd, FF, D),
    }
    return {k: v.astype(jnp.bfloat16) for k, v in drawn.items()}


def normed(x, gain):
    wide = x.astype(jnp.float32)
    scale = lax.rsqrt(jnp.mean(wide * wide, -1, keepdims=True) + 1e-6)
    return (wide * scale * gain.astype(jnp.float32)).astype(jnp.bfloat16)


def turned(t, place, theta):
    half = t.shape[-1] // 2
    angle = place.astype(jnp.float32)[:, None] * theta ** (-jnp.arange(half, dtype=jnp.float32) / half)
    cos, sin = jnp.cos(angle)[:, None], jnp.sin(angle)[:, None]
    a, b = t[..., :half].astype(jnp.float32), t[..., half:].astype(jnp.float32)
    return jnp.concatenate([a * cos - b * sin, b * cos + a * sin], -1).astype(jnp.bfloat16)


def matmul(a, w):
    return jnp.dot(a, w, preferred_element_type=jnp.float32).astype(jnp.bfloat16)


def einsum(form, a, b):
    return jnp.einsum(form, a.astype(jnp.float32), b.astype(jnp.float32))


def attention(q, k, v):
    scores = einsum("tgsd,ugd->gstu", q, k) * q.shape[-1] ** -0.5
    token = jnp.arange(q.shape[0])
    scores = jnp.where(token[:, None] >= token, scores, -jnp.inf)
    weights = jax.nn.softmax(scores, -1).astype(jnp.bfloat16)
    return einsum("gstu,ugd->tgsd", weights, v).astype(jnp.bfloat16)


def reference(x, gain_a, wq, wk, wv, wo, gain_m, w_gate, w_up, w_down):
    a, place = normed(x, gain_a), jnp.arange(ROWS)
    q = turned(matmul(a, wq).reshape(ROWS, HEADS, HEAD), place, THETA).reshape(ROWS, KV_HEADS, -1, HEAD)
    k = turned(matmul(a, wk).reshape(ROWS, KV_HEADS, HEAD), place, THETA)
    v = matmul(a, wv).reshape(ROWS, KV_HEADS, HEAD)
    seen = attention(q, k, v).reshape(ROWS, HEADS * HEAD)
    h = (x.astype(jnp.float32) + jnp.dot(seen, wo, preferred_element_type=jnp.float32)).astype(jnp.bfloat16)
    b = normed(h, gain_m)
    gate = jnp.dot(b, w_gate, preferred_element_type=jnp.float32)
    up = jnp.dot(b, w_up, preferred_element_type=jnp.float32)
    hidden = (jax.nn.silu(gate) * up).astype(jnp.bfloat16)
    return (h.astype(jnp.float32) + jnp.dot(hidden, w_down, preferred_element_type=jnp.float32)).astype(jnp.bfloat16)
```

```python
import functools

import jax
import jax.numpy as jnp
from jax import lax
from jax.experimental import pallas as pl
from jax.experimental.pallas import tpu as pltpu
from jax.sharding import PartitionSpec as P


HEAD = 128
THETA = 10000
LOG2E = 1.4426950408889634
NEG = -1e30
STRIP = 512
PART = 512
LAGS = (1, 2, 4)
SLOTS = 4
TILE = 256
DEPTH = 6144
PHASES = ((0, 256), (256, 768), (768, 1024))
F32, BF16 = jnp.float32, jnp.bfloat16


def _mxu(a, b, ca, cb):
    return lax.dot_general(a, b, (((ca,), (cb,)), ((), ())), preferred_element_type=F32)


def _turn(t, cos, sin):
    return t * cos + pltpu.roll(t, HEAD // 2, 1) * sin


def _attention(info_ref, q_ref, kv_ref, cos_ref, sin_ref, cosq_ref, sinq_ref, o_ref, q_s, k_s, v_s, top_s, mix_s, *, heads, blocks):
    own, step = HEAD, pl.program_id(0)
    group = 2 * own
    cols = heads * group
    me, core = info_ref[0], info_ref[1]
    whole = info_ref[2 + step]
    e = HEAD**-0.5 * LOG2E

    @pl.when(step == 0)
    def _():
        for r in range(blocks):
            rows = slice(r * own, (r + 1) * own)
            at = pl.ds(pl.multiple_of((me ^ r) * own, own), own)
            k_s[at, :] = _turn(kv_ref[rows, :HEAD].astype(F32), cos_ref[rows, :], sin_ref[rows, :]).astype(BF16)
            v_s[:HEAD, at] = kv_ref[rows, HEAD:].T
        v_s[HEAD:, :] = jnp.ones((8, blocks * own), BF16)

    cos, sin = cosq_ref[...], sinq_ref[...]
    for n in range(heads):
        q_s[n * group : (n + 1) * group, :] = _turn(q_ref[:, n * HEAD : (n + 1) * HEAD].astype(F32), cos, sin).astype(BF16)
    top_s[...] = jnp.full((1, cols), NEG, F32)
    mix_s[...] = jnp.zeros((HEAD + 8, cols), F32)
    strips = range(0, cols, STRIP)

    def block(j, masked):
        here = pl.ds(pl.multiple_of(j * group, group), group)
        keys, values = k_s[here, :], v_s[:, here]
        scores = [_mxu(keys, q_s[at : at + STRIP, :], 1, 1) for at in strips]
        if masked:
            query = lax.rem(lax.broadcasted_iota(jnp.int32, (group, STRIP), 1) + core * own, group)
            ok = query >= lax.broadcasted_iota(jnp.int32, (group, STRIP), 0)
        weights, keeps = [], []
        for at, s in zip(strips, scores):
            if masked:
                s = jnp.where(ok, s, 2 * NEG)
            old = top_s[:, at : at + STRIP]
            top = jnp.maximum(old, s.max(axis=0, keepdims=True))
            top_s[:, at : at + STRIP] = top
            weights.append(jnp.exp2((s - top) * e).astype(BF16))
            keeps.append(jnp.exp2((old - top) * e))
        for at, p, keep in zip(strips, weights, keeps):
            mix_s[:, at : at + STRIP] = mix_s[:, at : at + STRIP] * keep + _mxu(values, p, 1, 0)

    lax.fori_loop(0, whole, lambda j, _: block(j, False), None)
    block(whole, True)
    for at in strips:
        out = (mix_s[:HEAD, at : at + STRIP] * (1 / mix_s[HEAD : HEAD + 1, at : at + STRIP])).T.astype(BF16)
        for n in range(STRIP // group):
            head = at // group + n
            o_ref[:, head * HEAD : (head + 1) * HEAD] = out[n * group : (n + 1) * group, :]


def attention(q, kv, cos, sin, me, groups):
    rows, width = q.shape
    total = kv.shape[0]
    group, cols = 2 * HEAD, width * 2
    first = groups[0]
    info = jnp.stack([me, me % 2, *[(me // 2) ^ m for m in groups]]).astype(jnp.int32)
    whole = lambda g, _: (0, 0)
    mine = lambda g, _: (g, 0)
    table = lambda g, _: (first + g, 0)
    return pl.pallas_call(
        functools.partial(_attention, heads=width // HEAD, blocks=total // HEAD),
        grid_spec=pltpu.PrefetchScalarGridSpec(
            num_scalar_prefetch=1,
            grid=(rows // group,),
            in_specs=[pl.BlockSpec((group, width), mine), pl.BlockSpec((total, 2 * HEAD), whole), pl.BlockSpec((total, HEAD), whole),
                      pl.BlockSpec((total, HEAD), whole), pl.BlockSpec((group, HEAD), table), pl.BlockSpec((group, HEAD), table)],
            out_specs=pl.BlockSpec((group, width), mine),
            scratch_shapes=[pltpu.VMEM((cols, HEAD), BF16), pltpu.VMEM((total, HEAD), BF16), pltpu.VMEM((HEAD + 8, total), BF16),
                            pltpu.VMEM((1, cols), F32), pltpu.VMEM((HEAD + 8, cols), F32)],
        ),
        out_shape=jax.ShapeDtypeStruct((rows, width), BF16),
        compiler_params=pltpu.CompilerParams(dimension_semantics=("arbitrary",), vmem_limit_bytes=48 * 2**20),
        cost_estimate=pl.CostEstimate(flops=4 * rows * total * width, transcendentals=rows * total * width // HEAD, bytes_accessed=4 * rows * width),
    )(info, q, kv, cos, sin, cos, sin)


def normed(x, gain):
    wide = x.astype(F32)
    scale = lax.rsqrt(jnp.mean(wide * wide, -1, keepdims=True) + 1e-6)
    return (wide * scale * gain.astype(F32)).astype(BF16)


def tables(me, blocks, own):
    half = HEAD // 2
    place = ((me ^ jnp.arange(blocks))[:, None] * own + jnp.arange(own)).reshape(-1)
    angle = place.astype(F32)[:, None] * THETA ** (-jnp.arange(half, dtype=F32) / half)
    cos, sin = jnp.cos(angle), jnp.sin(angle)
    return jnp.concatenate([cos, cos], -1), jnp.concatenate([-sin, sin], -1)


def other(r):
    me = lax.axis_index("tp")
    out = me
    for bit in (1, 2, 4):
        if r & bit:
            out = out + bit - 2 * bit * lax.rem(lax.div(me, bit), 2)
    return out


def meet():
    barrier = pltpu.get_barrier_semaphore()
    for r in (1, 2, 4):
        pl.semaphore_signal(barrier, inc=1, device_id={"tp": other(r)}, device_id_type=pl.DeviceIdType.MESH)
    pl.semaphore_wait(barrier, 3)


def _gathered(x_ref, a_ref, b_ref, *rest, offset, steps, count, finish, outs, resident):
    extra, rest = rest[:resident], rest[resident:]
    out_refs, rest = rest[:outs], rest[outs:]
    xs, ws, acc, stage, kept, wsem, osem, ksem, own_sem, send, recv = rest
    own, depth = x_ref.shape
    half = own // 2
    meet()

    def copy(n, src, block, part, r):
        at = block * own + part * half
        return pltpu.make_async_remote_copy(src_ref=src, dst_ref=xs.at[pl.ds(at, half), :], send_sem=send.at[n], recv_sem=recv.at[n],
                                            device_id={"tp": other(r)}, device_id_type=pl.DeviceIdType.MESH)

    mine = lambda part: x_ref.at[pl.ds(part * half, half), :]
    held = lambda block, part: xs.at[pl.ds(block * own + part * half, half), :]
    partner = [copy(0, mine(0), 1, 0, 1), copy(1, mine(1), 1, 1, 1)]
    first = [copy(2, mine(0), 4, 0, 4), copy(3, mine(1), 2, 1, 2)]
    later = [copy(4, mine(1), 4, 1, 4), copy(5, mine(0), 2, 0, 2)]
    far = [copy(6, held(4, 0), 6, 0, 2), copy(7, held(2, 1), 6, 1, 4)]
    first_on = [copy(8, held(4, 0), 5, 0, 1), copy(9, held(2, 1), 3, 1, 1)]
    later_on = [copy(10, held(4, 1), 5, 1, 1), copy(11, held(2, 0), 3, 0, 1)]
    far_on = [copy(12, held(6, 0), 7, 0, 1), copy(13, held(6, 1), 7, 1, 1)]
    local = pltpu.make_async_copy(x_ref, xs.at[pl.ds(0, own), :], own_sem)

    def start(copies):
        for c in copies:
            c.start()

    def come(copies):
        for c in copies:
            c.wait_recv()

    def fetch(j, slot):
        at = pl.multiple_of(j * TILE, TILE)
        return [pltpu.make_async_copy(a_ref.at[:, pl.ds(at, TILE)], ws.at[slot, :, pl.ds(0, TILE)], wsem.at[slot, 0]),
                pltpu.make_async_copy(b_ref.at[:, pl.ds(offset + at, TILE)], ws.at[slot, :, pl.ds(TILE, TILE)], wsem.at[slot, 1])]

    stay = []
    at = 0
    for n, ref in enumerate(extra):
        stay.append(pltpu.make_async_copy(ref, kept.at[:, pl.ds(at, ref.shape[1])], ksem.at[n]))
        at += ref.shape[1]
    start(fetch(0, 0))
    start([local, *partner, *first, *later])
    start(stay)
    local.wait()
    come(partner)

    def product(rows, weights, width):
        low, high = rows
        acc[: high - low, :width] = jnp.zeros((high - low, width), F32)

        def add(k, _):
            at = pl.ds(pl.multiple_of(k * DEPTH, DEPTH), DEPTH)
            acc[: high - low, :width] += jnp.dot(xs[low:high, at], weights(at), preferred_element_type=F32)

        lax.fori_loop(0, depth // DEPTH, add, None)

    def put(rows, j, slot):
        low, high = rows
        return [pltpu.make_async_copy(stage.at[slot, pl.ds(0, high - low), pl.ds(s, w)], ref.at[pl.ds(low, high - low), pl.ds(pl.multiple_of(c + j * TILE, TILE), w)],
                                      osem.at[slot, n]) for n, (ref, s, w, c) in enumerate(finish(None, out_refs))]

    def run(rows, begin, end, base):
        size = rows[1] - rows[0]

        def one(j, _):
            slot = lax.rem(base + j, 2)
            for c in fetch(j, slot):
                c.wait()

            @pl.when(base + j + 1 < len(PHASES) * steps)
            def _():
                start(fetch(lax.rem(j + 1, steps), 1 - slot))

            product(rows, lambda at: ws[slot, at, :], 2 * TILE)

            @pl.when(j >= 2)
            def _():
                for c in put(rows, j - 2, lax.rem(j, 2)):
                    c.wait()

            stage[lax.rem(j, 2), :size, : finish.width] = finish(acc[:size, :], None)
            start(put(rows, j, lax.rem(j, 2)))

        lax.fori_loop(begin, end, one, None)

    def close(rows):
        for j in range(max(steps - 2, 0), steps):
            for c in put(rows, j, j % 2):
                c.wait()
        if resident:
            low, high = rows
            width = kept.shape[1]
            product(rows, lambda at: kept[at, :], width)
            stage[0, : high - low, :width] = acc[: high - low, :width].astype(BF16)
            c = pltpu.make_async_copy(stage.at[0, pl.ds(0, high - low), pl.ds(0, width)], out_refs[-1].at[pl.ds(low, high - low), :], osem.at[0, 0])
            c.start()
            c.wait()

    middle = min(count, steps)
    run(PHASES[0], 0, middle, 0)
    come(first)
    start([*far, *first_on])
    run(PHASES[0], middle, steps, 0)
    for c in stay:
        c.wait()
    close(PHASES[0])
    come(later)
    start(later_on)
    come([*first_on, *later_on])
    run(PHASES[1], 0, count, steps)
    come(far)
    start(far_on)
    run(PHASES[1], count, steps, steps)
    close(PHASES[1])
    come(far_on)
    run(PHASES[2], 0, steps, 2 * steps)
    close(PHASES[2])
    for c in [*partner, *first, *later, *far, *first_on, *later_on, *far_on]:
        c.wait_send()


class Plain:
    width = 2 * TILE

    def __init__(self, offset):
        self.offset = offset

    def __call__(self, acc, refs):
        if refs is not None:
            return [(refs[0], 0, TILE, 0), (refs[0], TILE, TILE, self.offset)]
        return acc.astype(BF16)


class Gated:
    width = TILE

    def __call__(self, acc, refs):
        if refs is not None:
            return [(refs[0], 0, TILE, 0)]
        return (jax.nn.silu(acc[:, :TILE]) * acc[:, TILE:]).astype(BF16)


def gathering(x, a, b, extra, shapes, finish, offset, steps, count, ident):
    own, depth = x.shape
    total = own * 8
    most = max(high - low for low, high in PHASES)
    wide = sum(t.shape[1] for t in extra)
    any_ = pl.BlockSpec(memory_space=pl.ANY)
    columns = 2 * TILE * steps + wide
    return pl.pallas_call(
        functools.partial(_gathered, offset=offset, steps=steps, count=count, finish=finish, outs=len(shapes), resident=len(extra)),
        in_specs=[any_] * (3 + len(extra)),
        out_specs=[any_] * len(shapes),
        out_shape=[jax.ShapeDtypeStruct((total, w), BF16) for w in shapes],
        scratch_shapes=[pltpu.VMEM((total, depth), BF16), pltpu.VMEM((2, depth, 2 * TILE), BF16), pltpu.VMEM((most, 2 * TILE), F32),
                        pltpu.VMEM((2, most, 2 * TILE), BF16), pltpu.VMEM((depth if extra else 16, wide or 128), BF16),
                        pltpu.SemaphoreType.DMA((2, 2)), pltpu.SemaphoreType.DMA((2, 2)), pltpu.SemaphoreType.DMA((2,)), pltpu.SemaphoreType.DMA,
                        pltpu.SemaphoreType.DMA((14,)), pltpu.SemaphoreType.DMA((14,))],
        compiler_params=pltpu.CompilerParams(collective_id=ident, has_side_effects=True, vmem_limit_bytes=63 * 2**20),
        cost_estimate=pl.CostEstimate(flops=2 * total * depth * columns, transcendentals=0, bytes_accessed=2 * depth * columns),
    )(x, a, b, *extra)


def _scattered(a_ref, w_ref, t_ref, y_ref, ws, even, c_out, f_out, s_out, c_in, f_in, s_in, wsem, c_send, f_send, s_send, c_recv, f_recv, s_recv):
    parts, own = c_in.shape[0], t_ref.shape[0]
    half = own // 2
    meet()

    def remote(src, dst, send, recv, r):
        return pltpu.make_async_remote_copy(src_ref=src, dst_ref=dst, send_sem=send, recv_sem=recv, device_id={"tp": other(r)}, device_id_type=pl.DeviceIdType.MESH)

    def core(j):
        s = lax.rem(j, 2)
        return [remote(c_out.at[s], c_in.at[j], c_send.at[s], c_recv.at[j], 1)]

    def far(j):
        s = lax.rem(j, SLOTS)
        return [remote(f_out.at[s, n], f_in.at[j, n], f_send.at[s, n], f_recv.at[j, n], r) for n, r in ((0, 4), (1, 2))]

    def side(j):
        s = lax.rem(j, SLOTS)
        return [remote(s_out.at[s, n], s_in.at[j, n], s_send.at[s, n], s_recv.at[j, n], r) for n, r in ((0, 4), (1, 2))]

    def fetch(j):
        s = lax.rem(j, 2)
        return pltpu.make_async_copy(w_ref.at[:, pl.ds(pl.multiple_of(j * PART, PART), PART)], ws.at[s], wsem.at[s])

    def sent(copies, j, slots):
        @pl.when(j >= slots)
        def _():
            for c in copies(jnp.maximum(j - slots, 0)):
                c.wait_send()

    def go(copies):
        for c in copies:
            c.start()

    def came(copies):
        for c in copies:
            c.wait_recv()

    fetch(0).start()
    keep = LAGS[-1] + 1

    def one(j, _):
        @pl.when(j < parts)
        def _():
            fetch(j).wait()

            @pl.when(j + 1 < parts)
            def _():
                fetch(j + 1).start()

            sent(core, j, 2)
            slot, at = lax.rem(j, 2), lax.rem(j, keep)

            def terms(m, _):
                low = pl.ds(pl.multiple_of(m * 2 * own, 2 * own), 2 * own)
                out = jnp.dot(a_ref[low, :], ws[slot], preferred_element_type=F32)
                even[at, m] = out[:own]
                c_out[slot, m] = out[own:].astype(BF16)

            lax.fori_loop(0, 4, terms, None)
            go(core(j))

        def later(lag, work):
            @pl.when((j >= lag) & (j - lag < parts))
            def _():
                work(j - lag)

        def first(p):
            came(core(p))
            sent(far, p, SLOTS)
            slot, at = lax.rem(p, SLOTS), lax.rem(p, keep)
            sum6 = (even[at, 3] + c_in[p, 3].astype(F32)).astype(BF16)
            f_out[slot, 0], f_out[slot, 1] = sum6[:half], sum6[half:]
            go(far(p))

        def second(p):
            came(far(p))
            sent(side, p, SLOTS)
            slot, at = lax.rem(p, SLOTS), lax.rem(p, keep)
            for n, m, plain, more in ((0, 2, slice(0, half), slice(half, own)), (1, 1, slice(half, own), slice(0, half))):
                s_out[slot, n, plain] = (even[at, m, plain] + c_in[p, m, plain].astype(F32)).astype(BF16)
                s_out[slot, n, more] = (even[at, m, more] + c_in[p, m, more].astype(F32) + f_in[p, 1 - n].astype(F32)).astype(BF16)
            go(side(p))

        def third(p):
            came(side(p))
            at = lax.rem(p, keep)
            cols = pl.ds(pl.multiple_of(p * PART, PART), PART)
            add = even[at, 0] + c_in[p, 0].astype(F32) + s_in[p, 0].astype(F32) + s_in[p, 1].astype(F32)
            y_ref[:, cols] = (t_ref[:, cols].astype(F32) + add).astype(BF16)

        for lag, work in zip(LAGS, (first, second, third)):
            later(lag, work)

    lax.fori_loop(0, parts + LAGS[-1], one, None)
    for copies, slots in ((core, 2), (far, SLOTS), (side, SLOTS)):
        for j in range(parts - slots, parts):
            for c in copies(j):
                c.wait_send()


def scattering(a, w, t, ident):
    own, d = t.shape
    depth, parts = a.shape[1], d // PART
    half = own // 2
    vmem = pl.BlockSpec(memory_space=pltpu.VMEM)
    dma = pltpu.SemaphoreType.DMA
    return pl.pallas_call(
        _scattered,
        in_specs=[vmem, pl.BlockSpec(memory_space=pl.ANY), vmem],
        out_specs=vmem,
        out_shape=jax.ShapeDtypeStruct((own, d), BF16),
        scratch_shapes=[pltpu.VMEM((2, depth, PART), BF16), pltpu.VMEM((LAGS[-1] + 1, 4, own, PART), F32), pltpu.VMEM((2, 4, own, PART), BF16),
                        pltpu.VMEM((SLOTS, 2, half, PART), BF16), pltpu.VMEM((SLOTS, 2, own, PART), BF16), pltpu.VMEM((parts, 4, own, PART), BF16),
                        pltpu.VMEM((parts, 2, half, PART), BF16), pltpu.VMEM((parts, 2, own, PART), BF16), dma((2,)), dma((2,)), dma((SLOTS, 2)),
                        dma((SLOTS, 2)), dma((parts,)), dma((parts, 2)), dma((parts, 2))],
        compiler_params=pltpu.CompilerParams(collective_id=ident, has_side_effects=True, vmem_limit_bytes=63 * 2**20),
        cost_estimate=pl.CostEstimate(flops=2 * a.shape[0] * depth * d, transcendentals=0, bytes_accessed=2 * depth * d),
    )(a, w, t)


def solution(mesh):
    n = mesh.shape["tp"]

    def step(x, gain_a, wq, wk, wv, wo, gain_m, w_gate, w_up, w_down):
        me = lax.axis_index("tp")
        cos, sin = tables(me, n, x.shape[0])
        half = wq.shape[1] // 2
        q, kv = gathering(normed(x, gain_a), wq, wq, (wk, wv), (2 * half, 2 * HEAD), Plain(half), half, half // TILE, half // TILE, 0)
        h = scattering(attention(q, kv, cos, sin, me, (0, 1, 2, 3)), wo, x, 1)
        hidden, = gathering(normed(h, gain_m), w_gate, w_up, (), (w_gate.shape[1],), Gated(), 0, w_gate.shape[1] // TILE, 10, 2)
        return scattering(hidden, w_down, h, 3)

    tokens, columns, rows_of = P(("dp", "tp"), None), P(None, "tp"), P("tp", None)
    return jax.shard_map(
        step,
        mesh=mesh,
        in_specs=(tokens, P(None), columns, columns, columns, rows_of, P(None), columns, columns, rows_of),
        out_specs=tokens,
        check_vma=False,
    )
```

```python
import functools

import jax
import jax.numpy as jnp
from jax import lax
from jax.experimental import pallas as pl
from jax.experimental.pallas import tpu as pltpu
from jax.sharding import PartitionSpec as P


HEAD = 128
THETA = 10000
LOG2E = 1.4426950408889634
NEG = -1e30
STRIP = 512
PART = 512
LAGS = (1, 2, 4)
SLOTS = 4
TILE = 256
DEPTH = 6144
NEAR, SIDE, FAR = (0, 256), (256, 768), (768, 1024)
BOTH = (256, 1024)
F32, BF16 = jnp.float32, jnp.bfloat16


def _mxu(a, b, ca, cb):
    return lax.dot_general(a, b, (((ca,), (cb,)), ((), ())), preferred_element_type=F32)


def _turn(t, cos, sin):
    return t * cos + pltpu.roll(t, HEAD // 2, 1) * sin


def _attention(info_ref, q_ref, kv_ref, cos_ref, sin_ref, cosq_ref, sinq_ref, o_ref, q_s, k_s, v_s, top_s, mix_s, *, heads, blocks):
    own, step = HEAD, pl.program_id(0)
    group = 2 * own
    cols = heads * group
    me, core = info_ref[0], info_ref[1]
    whole = info_ref[2 + step]
    e = HEAD**-0.5 * LOG2E

    @pl.when(step == 0)
    def _():
        for r in range(blocks):
            rows = slice(r * own, (r + 1) * own)
            at = pl.ds(pl.multiple_of((me ^ r) * own, own), own)
            k_s[at, :] = _turn(kv_ref[rows, :HEAD].astype(F32), cos_ref[rows, :], sin_ref[rows, :]).astype(BF16)
            v_s[:HEAD, at] = kv_ref[rows, HEAD:].T
        v_s[HEAD:, :] = jnp.ones((8, blocks * own), BF16)

    cos, sin = cosq_ref[...], sinq_ref[...]
    for n in range(heads):
        q_s[n * group : (n + 1) * group, :] = _turn(q_ref[:, n * HEAD : (n + 1) * HEAD].astype(F32), cos, sin).astype(BF16)
    top_s[...] = jnp.full((1, cols), NEG, F32)
    mix_s[...] = jnp.zeros((HEAD + 8, cols), F32)
    strips = range(0, cols, STRIP)

    def block(j, masked):
        here = pl.ds(pl.multiple_of(j * group, group), group)
        keys, values = k_s[here, :], v_s[:, here]
        scores = [_mxu(keys, q_s[at : at + STRIP, :], 1, 1) for at in strips]
        if masked:
            query = lax.rem(lax.broadcasted_iota(jnp.int32, (group, STRIP), 1) + core * own, group)
            ok = query >= lax.broadcasted_iota(jnp.int32, (group, STRIP), 0)
        weights, keeps = [], []
        for at, s in zip(strips, scores):
            if masked:
                s = jnp.where(ok, s, 2 * NEG)
            old = top_s[:, at : at + STRIP]
            top = jnp.maximum(old, s.max(axis=0, keepdims=True))
            top_s[:, at : at + STRIP] = top
            weights.append(jnp.exp2((s - top) * e).astype(BF16))
            keeps.append(jnp.exp2((old - top) * e))
        for at, p, keep in zip(strips, weights, keeps):
            mix_s[:, at : at + STRIP] = mix_s[:, at : at + STRIP] * keep + _mxu(values, p, 1, 0)

    lax.fori_loop(0, whole, lambda j, _: block(j, False), None)
    block(whole, True)
    for at in strips:
        out = (mix_s[:HEAD, at : at + STRIP] * (1 / mix_s[HEAD : HEAD + 1, at : at + STRIP])).T.astype(BF16)
        for n in range(STRIP // group):
            head = at // group + n
            o_ref[:, head * HEAD : (head + 1) * HEAD] = out[n * group : (n + 1) * group, :]


def attention(q, kv, cos, sin, me, groups):
    rows, width = q.shape
    total = kv.shape[0]
    group, cols = 2 * HEAD, width * 2
    first = groups[0]
    info = jnp.stack([me, me % 2, *[(me // 2) ^ m for m in groups]]).astype(jnp.int32)
    whole = lambda g, _: (0, 0)
    mine = lambda g, _: (g, 0)
    table = lambda g, _: (first + g, 0)
    return pl.pallas_call(
        functools.partial(_attention, heads=width // HEAD, blocks=total // HEAD),
        grid_spec=pltpu.PrefetchScalarGridSpec(
            num_scalar_prefetch=1,
            grid=(rows // group,),
            in_specs=[pl.BlockSpec((group, width), mine), pl.BlockSpec((total, 2 * HEAD), whole), pl.BlockSpec((total, HEAD), whole),
                      pl.BlockSpec((total, HEAD), whole), pl.BlockSpec((group, HEAD), table), pl.BlockSpec((group, HEAD), table)],
            out_specs=pl.BlockSpec((group, width), mine),
            scratch_shapes=[pltpu.VMEM((cols, HEAD), BF16), pltpu.VMEM((total, HEAD), BF16), pltpu.VMEM((HEAD + 8, total), BF16),
                            pltpu.VMEM((1, cols), F32), pltpu.VMEM((HEAD + 8, cols), F32)],
        ),
        out_shape=jax.ShapeDtypeStruct((rows, width), BF16),
        compiler_params=pltpu.CompilerParams(dimension_semantics=("arbitrary",), vmem_limit_bytes=48 * 2**20),
        cost_estimate=pl.CostEstimate(flops=4 * rows * total * width, transcendentals=rows * total * width // HEAD, bytes_accessed=4 * rows * width),
    )(info, q, kv, cos, sin, cos, sin)


def tables(me, blocks, own):
    half = HEAD // 2
    place = ((me ^ jnp.arange(blocks))[:, None] * own + jnp.arange(own)).reshape(-1)
    angle = place.astype(F32)[:, None] * THETA ** (-jnp.arange(half, dtype=F32) / half)
    cos, sin = jnp.cos(angle), jnp.sin(angle)
    return jnp.concatenate([cos, cos], -1), jnp.concatenate([-sin, sin], -1)


def other(r):
    me = lax.axis_index("tp")
    out = me
    for bit in (1, 2, 4):
        if r & bit:
            out = out + bit - 2 * bit * lax.rem(lax.div(me, bit), 2)
    return out


def meet():
    barrier = pltpu.get_barrier_semaphore()
    for r in (1, 2, 4):
        pl.semaphore_signal(barrier, inc=1, device_id={"tp": other(r)}, device_id_type=pl.DeviceIdType.MESH)
    pl.semaphore_wait(barrier, 3)


def _gathered(x_ref, gain_ref, a_ref, b_ref, *rest, offset, steps, count, alone, finish, outs, resident):
    extra, rest = rest[:resident], rest[resident:]
    out_refs, rest = rest[:outs], rest[outs:]
    xs, ws, acc, stage, kept, wsem, osem, ksem, send, recv = rest
    own, depth = x_ref.shape
    half = own // 2

    def fetch(j, slot):
        at = pl.multiple_of(j * TILE, TILE)
        return [pltpu.make_async_copy(a_ref.at[:, pl.ds(at, TILE)], ws.at[slot, :, pl.ds(0, TILE)], wsem.at[slot, 0]),
                pltpu.make_async_copy(b_ref.at[:, pl.ds(offset + at, TILE)], ws.at[slot, :, pl.ds(TILE, TILE)], wsem.at[slot, 1])]

    def start(copies):
        for c in copies:
            c.start()

    start(fetch(0, 0))
    pieces = [slice(at, at + 1024) for at in range(0, depth, 1024)]
    total = jnp.zeros((own, 1), F32)
    for at in pieces:
        wide = x_ref[:, at].astype(F32)
        total += jnp.sum(wide * wide, -1, keepdims=True)
    scale = lax.rsqrt(total * (1 / depth) + 1e-6)
    for at in pieces:
        xs[:own, at] = (x_ref[:, at].astype(F32) * scale * gain_ref[:, at].astype(F32)).astype(BF16)
    meet()

    def copy(n, src, block, part, r):
        at = block * own + part * half
        return pltpu.make_async_remote_copy(src_ref=src, dst_ref=xs.at[pl.ds(at, half), :], send_sem=send.at[n], recv_sem=recv.at[n],
                                            device_id={"tp": other(r)}, device_id_type=pl.DeviceIdType.MESH)

    mine = lambda part: xs.at[pl.ds(part * half, half), :]
    held = lambda block, part: xs.at[pl.ds(block * own + part * half, half), :]
    partner = [copy(0, mine(0), 1, 0, 1), copy(1, mine(1), 1, 1, 1)]
    first = [copy(2, mine(0), 4, 0, 4), copy(3, mine(1), 2, 1, 2)]
    later = [copy(4, mine(1), 4, 1, 4), copy(5, mine(0), 2, 0, 2)]
    far = [copy(6, held(4, 0), 6, 0, 2), copy(7, held(2, 1), 6, 1, 4)]
    first_on = [copy(8, held(4, 0), 5, 0, 1), copy(9, held(2, 1), 3, 1, 1)]
    later_on = [copy(10, held(4, 1), 5, 1, 1), copy(11, held(2, 0), 3, 0, 1)]
    far_on = [copy(12, held(6, 0), 7, 0, 1), copy(13, held(6, 1), 7, 1, 1)]

    def come(copies):
        for c in copies:
            c.wait_recv()

    stay = []
    at = 0
    for n, ref in enumerate(extra):
        stay.append(pltpu.make_async_copy(ref, kept.at[:, pl.ds(at, ref.shape[1])], ksem.at[n]))
        at += ref.shape[1]
    start([*partner, *first, *later])
    start(stay)
    come(partner)

    def product(rows, weights, width):
        low, high = rows
        acc[: high - low, :width] = jnp.zeros((high - low, width), F32)

        def add(k, _):
            at = pl.ds(pl.multiple_of(k * DEPTH, DEPTH), DEPTH)
            acc[: high - low, :width] += jnp.dot(xs[low:high, at], weights(at), preferred_element_type=F32)

        lax.fori_loop(0, depth // DEPTH, add, None)

    def put(rows, j, slot):
        low, high = rows
        return [pltpu.make_async_copy(stage.at[slot, pl.ds(0, high - low), pl.ds(s, w)], ref.at[pl.ds(low, high - low), pl.ds(pl.multiple_of(c + j * TILE, TILE), w)],
                                      osem.at[slot, n]) for n, (ref, s, w, c) in enumerate(finish(None, out_refs))]

    def run(rows, begin, end, base):
        size = rows[1] - rows[0]

        def one(j, _):
            slot = lax.rem(base + j - begin, 2)
            for c in fetch(j, slot):
                c.wait()

            @pl.when(base + j - begin + 1 < 2 * steps + alone)
            def _():
                start(fetch(lax.rem(j + 1, steps), 1 - slot))

            product(rows, lambda at: ws[slot, at, :], 2 * TILE)

            @pl.when(j >= begin + 2)
            def _():
                for c in put(rows, j - 2, lax.rem(j, 2)):
                    c.wait()

            stage[lax.rem(j, 2), :size, : finish.width] = finish(acc[:size, :], None)
            start(put(rows, j, lax.rem(j, 2)))

        if begin < end:
            lax.fori_loop(begin, end, one, None)
        for j in range(max(begin, end - 2), end):
            for c in put(rows, j, j % 2):
                c.wait()

    def close(rows):
        if resident:
            low, high = rows
            width = kept.shape[1]
            product(rows, lambda at: kept[at, :], width)
            stage[0, : high - low, :width] = acc[: high - low, :width].astype(BF16)
            c = pltpu.make_async_copy(stage.at[0, pl.ds(0, high - low), pl.ds(0, width)], out_refs[-1].at[pl.ds(low, high - low), :], osem.at[0, 0])
            c.start()
            c.wait()

    run(NEAR, 0, count, 0)
    come(first)
    start([*far, *first_on])
    run(NEAR, count, steps, count)
    for c in stay:
        c.wait()
    close(NEAR)
    come(later)
    start(later_on)
    come([*first_on, *later_on])
    run(SIDE, 0, alone - 1, steps)
    come(far)
    start(far_on)
    run(SIDE, alone - 1, alone, steps + alone - 1)
    close(SIDE)
    come(far_on)
    run(BOTH, alone, steps, steps + alone)
    run(FAR, 0, alone, 2 * steps)
    close(FAR)
    for c in [*partner, *first, *later, *far, *first_on, *later_on, *far_on]:
        c.wait_send()


class Plain:
    width = 2 * TILE

    def __init__(self, offset):
        self.offset = offset

    def __call__(self, acc, refs):
        if refs is not None:
            return [(refs[0], 0, TILE, 0), (refs[0], TILE, TILE, self.offset)]
        return acc.astype(BF16)


class Gated:
    width = TILE

    def __call__(self, acc, refs):
        if refs is not None:
            return [(refs[0], 0, TILE, 0)]
        return (jax.nn.silu(acc[:, :TILE]) * acc[:, TILE:]).astype(BF16)


def gathering(x, gain, a, b, extra, shapes, finish, offset, steps, count, alone, ident):
    own, depth = x.shape
    total = own * 8
    low, high = BOTH if alone < steps else SIDE
    most = high - low
    wide = sum(t.shape[1] for t in extra)
    any_ = pl.BlockSpec(memory_space=pl.ANY)
    columns = 2 * TILE * steps + wide
    return pl.pallas_call(
        functools.partial(_gathered, offset=offset, steps=steps, count=count, alone=alone, finish=finish, outs=len(shapes), resident=len(extra)),
        in_specs=[pl.BlockSpec(memory_space=pltpu.VMEM)] * 2 + [any_] * (2 + len(extra)),
        out_specs=[any_] * len(shapes),
        out_shape=[jax.ShapeDtypeStruct((total, w), BF16) for w in shapes],
        scratch_shapes=[pltpu.VMEM((total, depth), BF16), pltpu.VMEM((2, depth, 2 * TILE), BF16), pltpu.VMEM((most, 2 * TILE), F32),
                        pltpu.VMEM((2, most, 2 * TILE), BF16), pltpu.VMEM((depth if extra else 16, wide or 128), BF16),
                        pltpu.SemaphoreType.DMA((2, 2)), pltpu.SemaphoreType.DMA((2, 2)), pltpu.SemaphoreType.DMA((2,)),
                        pltpu.SemaphoreType.DMA((14,)), pltpu.SemaphoreType.DMA((14,))],
        compiler_params=pltpu.CompilerParams(collective_id=ident, has_side_effects=True, vmem_limit_bytes=63 * 2**20),
        cost_estimate=pl.CostEstimate(flops=2 * total * depth * columns, transcendentals=0, bytes_accessed=2 * depth * columns),
    )(x, gain.reshape(1, -1), a, b, *extra)


def _scattered(a_ref, w_ref, t_ref, y_ref, ws, even, c_out, f_out, s_out, c_in, f_in, s_in, wsem, c_send, f_send, s_send, c_recv, f_recv, s_recv):
    parts, own = c_in.shape[0], t_ref.shape[0]
    half = own // 2
    meet()

    def remote(src, dst, send, recv, r):
        return pltpu.make_async_remote_copy(src_ref=src, dst_ref=dst, send_sem=send, recv_sem=recv, device_id={"tp": other(r)}, device_id_type=pl.DeviceIdType.MESH)

    def core(j):
        s = lax.rem(j, 2)
        return [remote(c_out.at[s], c_in.at[j], c_send.at[s], c_recv.at[j], 1)]

    def far(j):
        s = lax.rem(j, SLOTS)
        return [remote(f_out.at[s, n], f_in.at[j, n], f_send.at[s, n], f_recv.at[j, n], r) for n, r in ((0, 4), (1, 2))]

    def side(j):
        s = lax.rem(j, SLOTS)
        return [remote(s_out.at[s, n], s_in.at[j, n], s_send.at[s, n], s_recv.at[j, n], r) for n, r in ((0, 4), (1, 2))]

    def fetch(j):
        s = lax.rem(j, 2)
        return pltpu.make_async_copy(w_ref.at[:, pl.ds(pl.multiple_of(j * PART, PART), PART)], ws.at[s], wsem.at[s])

    def sent(copies, j, slots):
        @pl.when(j >= slots)
        def _():
            for c in copies(jnp.maximum(j - slots, 0)):
                c.wait_send()

    def go(copies):
        for c in copies:
            c.start()

    def came(copies):
        for c in copies:
            c.wait_recv()

    fetch(0).start()
    keep = LAGS[-1] + 1

    def one(j, _):
        @pl.when(j < parts)
        def _():
            fetch(j).wait()

            @pl.when(j + 1 < parts)
            def _():
                fetch(j + 1).start()

            sent(core, j, 2)
            slot, at = lax.rem(j, 2), lax.rem(j, keep)

            for m in range(4):
                out = jnp.dot(a_ref[2 * m * own : 2 * (m + 1) * own, :], ws[slot], preferred_element_type=F32)
                even[at, m] = out[:own]
                c_out[slot, m] = out[own:].astype(BF16)

            go(core(j))

        def later(lag, work):
            @pl.when((j >= lag) & (j - lag < parts))
            def _():
                work(j - lag)

        def first(p):
            came(core(p))
            sent(far, p, SLOTS)
            slot, at = lax.rem(p, SLOTS), lax.rem(p, keep)
            sum6 = (even[at, 3] + c_in[p, 3].astype(F32)).astype(BF16)
            f_out[slot, 0], f_out[slot, 1] = sum6[:half], sum6[half:]
            go(far(p))

        def second(p):
            came(far(p))
            sent(side, p, SLOTS)
            slot, at = lax.rem(p, SLOTS), lax.rem(p, keep)
            for n, m, plain, more in ((0, 2, slice(0, half), slice(half, own)), (1, 1, slice(half, own), slice(0, half))):
                s_out[slot, n, plain] = (even[at, m, plain] + c_in[p, m, plain].astype(F32)).astype(BF16)
                s_out[slot, n, more] = (even[at, m, more] + c_in[p, m, more].astype(F32) + f_in[p, 1 - n].astype(F32)).astype(BF16)
            go(side(p))

        def third(p):
            came(side(p))
            at = lax.rem(p, keep)
            cols = pl.ds(pl.multiple_of(p * PART, PART), PART)
            add = even[at, 0] + c_in[p, 0].astype(F32) + s_in[p, 0].astype(F32) + s_in[p, 1].astype(F32)
            y_ref[:, cols] = (t_ref[:, cols].astype(F32) + add).astype(BF16)

        for lag, work in zip(LAGS, (first, second, third)):
            later(lag, work)

    lax.fori_loop(0, parts + LAGS[-1], one, None)
    for copies, slots in ((core, 2), (far, SLOTS), (side, SLOTS)):
        for j in range(parts - slots, parts):
            for c in copies(j):
                c.wait_send()


def scattering(a, w, t, ident):
    own, d = t.shape
    depth, parts = a.shape[1], d // PART
    half = own // 2
    vmem = pl.BlockSpec(memory_space=pltpu.VMEM)
    dma = pltpu.SemaphoreType.DMA
    return pl.pallas_call(
        _scattered,
        in_specs=[vmem, pl.BlockSpec(memory_space=pl.ANY), vmem],
        out_specs=vmem,
        out_shape=jax.ShapeDtypeStruct((own, d), BF16),
        scratch_shapes=[pltpu.VMEM((2, depth, PART), BF16), pltpu.VMEM((LAGS[-1] + 1, 4, own, PART), F32), pltpu.VMEM((2, 4, own, PART), BF16),
                        pltpu.VMEM((SLOTS, 2, half, PART), BF16), pltpu.VMEM((SLOTS, 2, own, PART), BF16), pltpu.VMEM((parts, 4, own, PART), BF16),
                        pltpu.VMEM((parts, 2, half, PART), BF16), pltpu.VMEM((parts, 2, own, PART), BF16), dma((2,)), dma((2,)), dma((SLOTS, 2)),
                        dma((SLOTS, 2)), dma((parts,)), dma((parts, 2)), dma((parts, 2))],
        compiler_params=pltpu.CompilerParams(collective_id=ident, has_side_effects=True, vmem_limit_bytes=63 * 2**20),
        cost_estimate=pl.CostEstimate(flops=2 * a.shape[0] * depth * d, transcendentals=0, bytes_accessed=2 * depth * d),
    )(a, w, t)


def solution(mesh):
    n = mesh.shape["tp"]

    def step(x, gain_a, wq, wk, wv, wo, gain_m, w_gate, w_up, w_down):
        me = lax.axis_index("tp")
        cos, sin = tables(me, n, x.shape[0])
        half = wq.shape[1] // 2
        q, kv = gathering(x, gain_a, wq, wq, (wk, wv), (2 * half, 2 * HEAD), Plain(half), half, half // TILE, half // TILE, half // TILE, 0)
        h = scattering(attention(q, kv, cos, sin, me, (0, 1, 2, 3)), wo, x, 1)
        hidden, = gathering(h, gain_m, w_gate, w_up, (), (w_gate.shape[1],), Gated(), 0, w_gate.shape[1] // TILE, 10, 5, 2)
        return scattering(hidden, w_down, h, 3)

    tokens, columns, rows_of = P(("dp", "tp"), None), P(None, "tp"), P("tp", None)
    return jax.shard_map(
        step,
        mesh=mesh,
        in_specs=(tokens, P(None), columns, columns, columns, rows_of, P(None), columns, columns, rows_of),
        out_specs=tokens,
        check_vma=False,
    )
```

```python
import functools

import jax
import jax.numpy as jnp
from jax import lax
from jax.experimental import pallas as pl
from jax.experimental.pallas import tpu as pltpu
from jax.sharding import PartitionSpec as P


HEAD = 128
THETA = 10000
LOG2E = 1.4426950408889634
NEG = -1e30
STRIP = 512
PART = 512
LAGS = (1, 2, 4)
SLOTS = 4
TILE = 256
DEPTH = 6144
NEAR, SIDE, FAR = (0, 256), (256, 768), (768, 1024)
BOTH = (256, 1024)
F32, BF16 = jnp.float32, jnp.bfloat16


def _mxu(a, b, ca, cb):
    return lax.dot_general(a, b, (((ca,), (cb,)), ((), ())), preferred_element_type=F32)


def _turn(t, cos, sin):
    return t * cos + pltpu.roll(t, HEAD // 2, 1) * sin


def _attention(info_ref, q_ref, kv_ref, cos_ref, sin_ref, cosq_ref, sinq_ref, o_ref, q_s, k_s, v_s, top_s, mix_s, *, heads, blocks):
    own, step = HEAD, pl.program_id(0)
    group = 2 * own
    cols = heads * group
    me, core = info_ref[0], info_ref[1]
    whole = info_ref[2 + step]
    e = HEAD**-0.5 * LOG2E

    @pl.when(step == 0)
    def _():
        for r in range(blocks):
            rows = slice(r * own, (r + 1) * own)
            at = pl.ds(pl.multiple_of((me ^ r) * own, own), own)
            k_s[at, :] = _turn(kv_ref[rows, :HEAD].astype(F32), cos_ref[rows, :], sin_ref[rows, :]).astype(BF16)
            v_s[:HEAD, at] = kv_ref[rows, HEAD:].T
        v_s[HEAD:, :] = jnp.ones((8, blocks * own), BF16)

    cos, sin = cosq_ref[...], sinq_ref[...]
    for n in range(heads):
        q_s[n * group : (n + 1) * group, :] = _turn(q_ref[:, n * HEAD : (n + 1) * HEAD].astype(F32), cos, sin).astype(BF16)
    top_s[...] = jnp.full((1, cols), NEG, F32)
    mix_s[...] = jnp.zeros((HEAD + 8, cols), F32)
    strips = range(0, cols, STRIP)

    def block(j, masked):
        here = pl.ds(pl.multiple_of(j * group, group), group)
        keys, values = k_s[here, :], v_s[:, here]
        scores = [_mxu(keys, q_s[at : at + STRIP, :], 1, 1) for at in strips]
        if masked:
            query = lax.rem(lax.broadcasted_iota(jnp.int32, (group, STRIP), 1) + core * own, group)
            ok = query >= lax.broadcasted_iota(jnp.int32, (group, STRIP), 0)
        weights, keeps = [], []
        for at, s in zip(strips, scores):
            if masked:
                s = jnp.where(ok, s, 2 * NEG)
            old = top_s[:, at : at + STRIP]
            top = jnp.maximum(old, s.max(axis=0, keepdims=True))
            top_s[:, at : at + STRIP] = top
            weights.append(jnp.exp2((s - top) * e).astype(BF16))
            keeps.append(jnp.exp2((old - top) * e))
        for at, p, keep in zip(strips, weights, keeps):
            mix_s[:, at : at + STRIP] = mix_s[:, at : at + STRIP] * keep + _mxu(values, p, 1, 0)

    lax.fori_loop(0, whole, lambda j, _: block(j, False), None)
    block(whole, True)
    for at in strips:
        out = (mix_s[:HEAD, at : at + STRIP] * (1 / mix_s[HEAD : HEAD + 1, at : at + STRIP])).T.astype(BF16)
        for n in range(STRIP // group):
            head = at // group + n
            o_ref[:, head * HEAD : (head + 1) * HEAD] = out[n * group : (n + 1) * group, :]


def attention(q, kv, cos, sin, me, groups):
    rows, width = q.shape
    total = kv.shape[0]
    group, cols = 2 * HEAD, width * 2
    first = groups[0]
    info = jnp.stack([me, me % 2, *[(me // 2) ^ m for m in groups]]).astype(jnp.int32)
    whole = lambda g, _: (0, 0)
    mine = lambda g, _: (g, 0)
    table = lambda g, _: (first + g, 0)
    return pl.pallas_call(
        functools.partial(_attention, heads=width // HEAD, blocks=total // HEAD),
        grid_spec=pltpu.PrefetchScalarGridSpec(
            num_scalar_prefetch=1,
            grid=(rows // group,),
            in_specs=[pl.BlockSpec((group, width), mine), pl.BlockSpec((total, 2 * HEAD), whole), pl.BlockSpec((total, HEAD), whole),
                      pl.BlockSpec((total, HEAD), whole), pl.BlockSpec((group, HEAD), table), pl.BlockSpec((group, HEAD), table)],
            out_specs=pl.BlockSpec((group, width), mine),
            scratch_shapes=[pltpu.VMEM((cols, HEAD), BF16), pltpu.VMEM((total, HEAD), BF16), pltpu.VMEM((HEAD + 8, total), BF16),
                            pltpu.VMEM((1, cols), F32), pltpu.VMEM((HEAD + 8, cols), F32)],
        ),
        out_shape=jax.ShapeDtypeStruct((rows, width), BF16),
        compiler_params=pltpu.CompilerParams(dimension_semantics=("arbitrary",), vmem_limit_bytes=48 * 2**20),
        cost_estimate=pl.CostEstimate(flops=4 * rows * total * width, transcendentals=rows * total * width // HEAD, bytes_accessed=4 * rows * width),
    )(info, q, kv, cos, sin, cos, sin)


def tables(me, blocks, own):
    half = HEAD // 2
    place = ((me ^ jnp.arange(blocks))[:, None] * own + jnp.arange(own)).reshape(-1)
    angle = place.astype(F32)[:, None] * THETA ** (-jnp.arange(half, dtype=F32) / half)
    cos, sin = jnp.cos(angle), jnp.sin(angle)
    return jnp.concatenate([cos, cos], -1), jnp.concatenate([-sin, sin], -1)


def other(r):
    me = lax.axis_index("tp")
    out = me
    for bit in (1, 2, 4):
        if r & bit:
            out = out + bit - 2 * bit * lax.rem(lax.div(me, bit), 2)
    return out


def meet():
    barrier = pltpu.get_barrier_semaphore()
    for r in (1, 2, 4):
        pl.semaphore_signal(barrier, inc=1, device_id={"tp": other(r)}, device_id_type=pl.DeviceIdType.MESH)
    pl.semaphore_wait(barrier, 3)


def _gathered(x_ref, gain_ref, a_ref, b_ref, *rest, offset, steps, count, alone, finish, outs, resident):
    extra, rest = rest[:resident], rest[resident:]
    out_refs, rest = rest[:outs], rest[outs:]
    xs, ws, acc, stage, kept, wsem, osem, ksem, send, recv = rest
    own, depth = x_ref.shape
    half = own // 2

    def fetch(j, slot):
        at = pl.multiple_of(j * TILE, TILE)
        return [pltpu.make_async_copy(a_ref.at[:, pl.ds(at, TILE)], ws.at[slot, :, pl.ds(0, TILE)], wsem.at[slot, 0]),
                pltpu.make_async_copy(b_ref.at[:, pl.ds(offset + at, TILE)], ws.at[slot, :, pl.ds(TILE, TILE)], wsem.at[slot, 1])]

    def start(copies):
        for c in copies:
            c.start()

    start(fetch(0, 0))
    pieces = [slice(at, at + 1024) for at in range(0, depth, 1024)]
    total = jnp.zeros((own, 1), F32)
    for at in pieces:
        wide = x_ref[:, at].astype(F32)
        total += jnp.sum(wide * wide, -1, keepdims=True)
    scale = lax.rsqrt(total * (1 / depth) + 1e-6)
    for at in pieces:
        xs[:own, at] = (x_ref[:, at].astype(F32) * scale * gain_ref[at].astype(F32)[None]).astype(BF16)
    meet()

    def copy(n, src, block, part, r):
        at = block * own + part * half
        return pltpu.make_async_remote_copy(src_ref=src, dst_ref=xs.at[pl.ds(at, half), :], send_sem=send.at[n], recv_sem=recv.at[n],
                                            device_id={"tp": other(r)}, device_id_type=pl.DeviceIdType.MESH)

    mine = lambda part: xs.at[pl.ds(part * half, half), :]
    held = lambda block, part: xs.at[pl.ds(block * own + part * half, half), :]
    partner = [copy(0, mine(0), 1, 0, 1), copy(1, mine(1), 1, 1, 1)]
    first = [copy(2, mine(0), 4, 0, 4), copy(3, mine(1), 2, 1, 2)]
    later = [copy(4, mine(1), 4, 1, 4), copy(5, mine(0), 2, 0, 2)]
    far = [copy(6, held(4, 0), 6, 0, 2), copy(7, held(2, 1), 6, 1, 4)]
    first_on = [copy(8, held(4, 0), 5, 0, 1), copy(9, held(2, 1), 3, 1, 1)]
    later_on = [copy(10, held(4, 1), 5, 1, 1), copy(11, held(2, 0), 3, 0, 1)]
    far_on = [copy(12, held(6, 0), 7, 0, 1), copy(13, held(6, 1), 7, 1, 1)]

    def come(copies):
        for c in copies:
            c.wait_recv()

    stay = []
    at = 0
    for n, ref in enumerate(extra):
        stay.append(pltpu.make_async_copy(ref, kept.at[:, pl.ds(at, ref.shape[1])], ksem.at[n]))
        at += ref.shape[1]
    start([*partner, *first, *later])
    start(stay)
    come(partner)

    def product(rows, weights, width):
        low, high = rows
        acc[: high - low, :width] = jnp.zeros((high - low, width), F32)

        def add(k, _):
            at = pl.ds(pl.multiple_of(k * DEPTH, DEPTH), DEPTH)
            acc[: high - low, :width] += jnp.dot(xs[low:high, at], weights(at), preferred_element_type=F32)

        lax.fori_loop(0, depth // DEPTH, add, None)

    def put(rows, j, slot):
        low, high = rows
        return [pltpu.make_async_copy(stage.at[slot, pl.ds(0, high - low), pl.ds(s, w)], ref.at[pl.ds(low, high - low), pl.ds(pl.multiple_of(c + j * TILE, TILE), w)],
                                      osem.at[slot, n]) for n, (ref, s, w, c) in enumerate(finish(None, out_refs))]

    def run(rows, begin, end, base):
        size = rows[1] - rows[0]

        def one(j, _):
            slot = lax.rem(base + j - begin, 2)
            for c in fetch(j, slot):
                c.wait()

            @pl.when(base + j - begin + 1 < 2 * steps + alone)
            def _():
                start(fetch(lax.rem(j + 1, steps), 1 - slot))

            product(rows, lambda at: ws[slot, at, :], 2 * TILE)

            @pl.when(j >= begin + 2)
            def _():
                for c in put(rows, j - 2, lax.rem(j, 2)):
                    c.wait()

            stage[lax.rem(j, 2), :size, : finish.width] = finish(acc[:size, :], None)
            start(put(rows, j, lax.rem(j, 2)))

        if begin < end:
            lax.fori_loop(begin, end, one, None)
        for j in range(max(begin, end - 2), end):
            for c in put(rows, j, j % 2):
                c.wait()

    def close(rows):
        if resident:
            low, high = rows
            width = kept.shape[1]
            product(rows, lambda at: kept[at, :], width)
            stage[0, : high - low, :width] = acc[: high - low, :width].astype(BF16)
            c = pltpu.make_async_copy(stage.at[0, pl.ds(0, high - low), pl.ds(0, width)], out_refs[-1].at[pl.ds(low, high - low), :], osem.at[0, 0])
            c.start()
            c.wait()

    run(NEAR, 0, count, 0)
    come(first)
    start([*far, *first_on])
    run(NEAR, count, steps, count)
    for c in stay:
        c.wait()
    close(NEAR)
    come(later)
    start(later_on)
    come([*first_on, *later_on])
    early = alone - 1 if alone < steps else alone
    run(SIDE, 0, early, steps)
    come(far)
    start(far_on)
    run(SIDE, early, alone, steps + early)
    close(SIDE)
    come(far_on)
    run(BOTH, alone, steps, steps + alone)
    run(FAR, 0, alone, 2 * steps)
    close(FAR)
    for c in [*partner, *first, *later, *far, *first_on, *later_on, *far_on]:
        c.wait_send()


class Plain:
    width = 2 * TILE

    def __init__(self, offset):
        self.offset = offset

    def __call__(self, acc, refs):
        if refs is not None:
            return [(refs[0], 0, TILE, 0), (refs[0], TILE, TILE, self.offset)]
        return acc.astype(BF16)


class Gated:
    width = TILE

    def __call__(self, acc, refs):
        if refs is not None:
            return [(refs[0], 0, TILE, 0)]
        return (jax.nn.silu(acc[:, :TILE]) * acc[:, TILE:]).astype(BF16)


def gathering(x, gain, a, b, extra, shapes, finish, offset, steps, count, alone, ident):
    own, depth = x.shape
    total = own * 8
    low, high = BOTH if alone < steps else SIDE
    most = high - low
    wide = sum(t.shape[1] for t in extra)
    any_ = pl.BlockSpec(memory_space=pl.ANY)
    columns = 2 * TILE * steps + wide
    return pl.pallas_call(
        functools.partial(_gathered, offset=offset, steps=steps, count=count, alone=alone, finish=finish, outs=len(shapes), resident=len(extra)),
        in_specs=[pl.BlockSpec(memory_space=pltpu.VMEM)] * 2 + [any_] * (2 + len(extra)),
        out_specs=[any_] * len(shapes),
        out_shape=[jax.ShapeDtypeStruct((total, w), BF16) for w in shapes],
        scratch_shapes=[pltpu.VMEM((total, depth), BF16), pltpu.VMEM((2, depth, 2 * TILE), BF16), pltpu.VMEM((most, 2 * TILE), F32),
                        pltpu.VMEM((2, most, 2 * TILE), BF16), pltpu.VMEM((depth if extra else 16, wide or 128), BF16),
                        pltpu.SemaphoreType.DMA((2, 2)), pltpu.SemaphoreType.DMA((2, 2)), pltpu.SemaphoreType.DMA((2,)),
                        pltpu.SemaphoreType.DMA((14,)), pltpu.SemaphoreType.DMA((14,))],
        compiler_params=pltpu.CompilerParams(collective_id=ident, has_side_effects=True, vmem_limit_bytes=63 * 2**20),
        cost_estimate=pl.CostEstimate(flops=2 * total * depth * columns, transcendentals=0, bytes_accessed=2 * depth * columns),
    )(x, gain, a, b, *extra)


def _scattered(a_ref, w_ref, t_ref, y_ref, ws, even, c_out, f_out, s_out, c_in, f_in, s_in, wsem, c_send, f_send, s_send, c_recv, f_recv, s_recv):
    parts, own = c_in.shape[0], t_ref.shape[0]
    half = own // 2
    meet()

    def remote(src, dst, send, recv, r):
        return pltpu.make_async_remote_copy(src_ref=src, dst_ref=dst, send_sem=send, recv_sem=recv, device_id={"tp": other(r)}, device_id_type=pl.DeviceIdType.MESH)

    def core(j):
        s = lax.rem(j, 2)
        return [remote(c_out.at[s], c_in.at[j], c_send.at[s], c_recv.at[j], 1)]

    def far(j):
        s = lax.rem(j, SLOTS)
        return [remote(f_out.at[s, n], f_in.at[j, n], f_send.at[s, n], f_recv.at[j, n], r) for n, r in ((0, 4), (1, 2))]

    def side(j):
        s = lax.rem(j, SLOTS)
        return [remote(s_out.at[s, n], s_in.at[j, n], s_send.at[s, n], s_recv.at[j, n], r) for n, r in ((0, 4), (1, 2))]

    def fetch(j):
        s = lax.rem(j, 2)
        return pltpu.make_async_copy(w_ref.at[:, pl.ds(pl.multiple_of(j * PART, PART), PART)], ws.at[s], wsem.at[s])

    def sent(copies, j, slots):
        @pl.when(j >= slots)
        def _():
            for c in copies(jnp.maximum(j - slots, 0)):
                c.wait_send()

    def go(copies):
        for c in copies:
            c.start()

    def came(copies):
        for c in copies:
            c.wait_recv()

    fetch(0).start()
    keep = LAGS[-1] + 1

    def one(j, _):
        @pl.when(j < parts)
        def _():
            fetch(j).wait()

            @pl.when(j + 1 < parts)
            def _():
                fetch(j + 1).start()

            sent(core, j, 2)
            slot, at = lax.rem(j, 2), lax.rem(j, keep)

            for m in range(4):
                out = jnp.dot(a_ref[2 * m * own : 2 * (m + 1) * own, :], ws[slot], preferred_element_type=F32)
                even[at, m] = out[:own]
                c_out[slot, m] = out[own:].astype(BF16)

            go(core(j))

        def later(lag, work):
            @pl.when((j >= lag) & (j - lag < parts))
            def _():
                work(j - lag)

        def first(p):
            came(core(p))
            sent(far, p, SLOTS)
            slot, at = lax.rem(p, SLOTS), lax.rem(p, keep)
            sum6 = (even[at, 3] + c_in[p, 3].astype(F32)).astype(BF16)
            f_out[slot, 0], f_out[slot, 1] = sum6[:half], sum6[half:]
            go(far(p))

        def second(p):
            came(far(p))
            sent(side, p, SLOTS)
            slot, at = lax.rem(p, SLOTS), lax.rem(p, keep)
            for n, m, plain, more in ((0, 2, slice(0, half), slice(half, own)), (1, 1, slice(half, own), slice(0, half))):
                s_out[slot, n, plain] = (even[at, m, plain] + c_in[p, m, plain].astype(F32)).astype(BF16)
                s_out[slot, n, more] = (even[at, m, more] + c_in[p, m, more].astype(F32) + f_in[p, 1 - n].astype(F32)).astype(BF16)
            go(side(p))

        def third(p):
            came(side(p))
            at = lax.rem(p, keep)
            cols = pl.ds(pl.multiple_of(p * PART, PART), PART)
            add = even[at, 0] + c_in[p, 0].astype(F32) + s_in[p, 0].astype(F32) + s_in[p, 1].astype(F32)
            y_ref[:, cols] = (t_ref[:, cols].astype(F32) + add).astype(BF16)

        for lag, work in zip(LAGS, (first, second, third)):
            later(lag, work)

    lax.fori_loop(0, parts + LAGS[-1], one, None)
    for copies, slots in ((core, 2), (far, SLOTS), (side, SLOTS)):
        for j in range(parts - slots, parts):
            for c in copies(j):
                c.wait_send()


def scattering(a, w, t, ident):
    own, d = t.shape
    depth, parts = a.shape[1], d // PART
    half = own // 2
    vmem = pl.BlockSpec(memory_space=pltpu.VMEM)
    dma = pltpu.SemaphoreType.DMA
    return pl.pallas_call(
        _scattered,
        in_specs=[vmem, pl.BlockSpec(memory_space=pl.ANY), vmem],
        out_specs=vmem,
        out_shape=jax.ShapeDtypeStruct((own, d), BF16),
        scratch_shapes=[pltpu.VMEM((2, depth, PART), BF16), pltpu.VMEM((LAGS[-1] + 1, 4, own, PART), F32), pltpu.VMEM((2, 4, own, PART), BF16),
                        pltpu.VMEM((SLOTS, 2, half, PART), BF16), pltpu.VMEM((SLOTS, 2, own, PART), BF16), pltpu.VMEM((parts, 4, own, PART), BF16),
                        pltpu.VMEM((parts, 2, half, PART), BF16), pltpu.VMEM((parts, 2, own, PART), BF16), dma((2,)), dma((2,)), dma((SLOTS, 2)),
                        dma((SLOTS, 2)), dma((parts,)), dma((parts, 2)), dma((parts, 2))],
        compiler_params=pltpu.CompilerParams(collective_id=ident, has_side_effects=True, vmem_limit_bytes=63 * 2**20),
        cost_estimate=pl.CostEstimate(flops=2 * a.shape[0] * depth * d, transcendentals=0, bytes_accessed=2 * depth * d),
    )(a, w, t)


def solution(mesh):
    n = mesh.shape["tp"]

    def step(x, gain_a, wq, wk, wv, wo, gain_m, w_gate, w_up, w_down):
        me = lax.axis_index("tp")
        cos, sin = tables(me, n, x.shape[0])
        half = wq.shape[1] // 2
        q, kv = gathering(x, gain_a, wq, wq, (wk, wv), (2 * half, 2 * HEAD), Plain(half), half, half // TILE, half // TILE, half // TILE, 0)
        h = scattering(attention(q, kv, cos, sin, me, (0, 1, 2, 3)), wo, x, 1)
        hidden, = gathering(h, gain_m, w_gate, w_up, (), (w_gate.shape[1],), Gated(), 0, w_gate.shape[1] // TILE, 10, 5, 2)
        return scattering(hidden, w_down, h, 3)

    tokens, columns, rows_of = P(("dp", "tp"), None), P(None, "tp"), P("tp", None)
    return jax.shard_map(
        step,
        mesh=mesh,
        in_specs=(tokens, P(None), columns, columns, columns, rows_of, P(None), columns, columns, rows_of),
        out_specs=tokens,
        check_vma=False,
    )
```
